32 devices in a mesh: dp: 8 (over z, x), mp: 4 (over y, core).
Axes of the slice: x: 2, y: 2, z: 4, core: 2. Of those that a mesh axis runs over, the one named last changes fastest.
Arguments:
- hidden: bfloat16 [2048, 8192], P('dp', 'mp'), may hold values from -6 to 6
- norm_gain: bfloat16 [8192], P('mp'), may hold values from 0.5 to 1.5
- kv_weight: bfloat16 [8192, 2048], P(None, 'mp'), may hold values from -0.0625 to 0.0625
- clip_upper: float32 [64, 2048], P(None, 'mp'), may hold values from 0.5 to 4
- clip_lower: float32 [64, 2048], P(None, 'mp'), may hold values from 0.5 to 4
Outputs:
- upper_final: float32 [64, 2048], P('dp', 'mp')
- lower_final: float32 [64, 2048], P('dp', 'mp')
The draws below stay inside these ranges and needn't reach their ends.
All inputs are finite; a program needn't handle non-finite values.
Results may differ from the reference program's by a relative error of at most 0.012.
Values may be sent and summed in bfloat16 or wider, within the bound.
A program may use at most 64 MiB of HBM per device.

```python
import math
import jax
import jax.numpy as jnp
from jax import lax

D = 8192
KVW = 1024
GROUP = 128
STEPS = 2
TOKENS = 2048
GROUPS = 64


def block_scale(key, dims, cuts, smallest, high):
    def one(axis_at, shards_of):
        heights = jax.random.uniform(jax.random.fold_in(jax.random.fold_in(key, 6), axis_at), (shards_of,), jnp.float32, smallest / len(cuts), high / len(cuts))
        return jnp.repeat(jnp.exp(heights), dims[axis_at] // shards_of).reshape((-1,) + (1,) * (len(dims) - axis_at - 1))

    level = one(*cuts[0])
    for cut in cuts[1:]:
        level = level * one(*cut)
    return level


def centred(own_key, extent, width, most, cuts=(), held_as=jnp.bfloat16):
    array = jax.random.normal(own_key, extent, jnp.float32) * width
    if len(cuts) > 0:
        array = block_scale(own_key, extent, cuts, -0.22, 0.18) * array
    return jnp.clip(array, min=-most, max=most).astype(held_as)


def setup_inputs(seed: int = 0) -> dict:
    seeds = jax.random.split(jax.random.key(seed), 6)
    return {
        "hidden": centred(seeds[0], (TOKENS, D), 1.0, 6.0, ((0, 8), (1, 4))),
        "norm_gain": jnp.clip(1.0 + 0.1 * jax.random.normal(seeds[1], (D,), jnp.float32), 0.5, 1.5).astype(jnp.bfloat16),
        "kv_weight": centred(seeds[2], (D, 2 * KVW), D ** -0.5, 0.0625, ((1, 4),)),
        "clip_upper": jnp.clip(0.5 + 3.5 * jax.random.uniform(seeds[3], (GROUPS, 2 * KVW), jnp.float32) ** block_scale(seeds[3], (GROUPS, 2 * KVW), ((1, 4),), -0.2, 0.2), 0.5, 4.0),
        "clip_lower": jnp.clip(0.5 + 3.5 * jax.random.uniform(seeds[4], (GROUPS, 2 * KVW), jnp.float32) ** block_scale(seeds[4], (GROUPS, 2 * KVW), ((1, 4),), -0.2, 0.2), 0.5, 4.0),
    }


norm_eps = 1e-05
grad_eps = 1e-06
learn_rate = 0.25
top_level = 15.0
two_pi = 2.0 * math.pi

def fake_quant(upper, lower, grouped, magnitude):
    top_clip = jax.nn.sigmoid(upper) * magnitude
    bottom_clip = jax.nn.sigmoid(lower) * magnitude
    quant_step = (top_clip + bottom_clip + 1e-06) / top_level
    zero_point = bottom_clip / quant_step
    level = jnp.clip(grouped / quant_step[:, None, :] + zero_point[:, None, :], 0.0, top_level)
    soft_level = level - jnp.sin(two_pi * level) / two_pi
    fake = (soft_level - zero_point[:, None, :]) * quant_step[:, None, :]
    return fake.reshape(grouped.shape[0] * grouped.shape[1], grouped.shape[2])

def clip_gradients(upper, lower, grouped, magnitude, normed, targets):

    def quantizer(first, second):
        return fake_quant(first, second, grouped, magnitude)
    fake, pullback = jax.vjp(quantizer, upper, lower)
    quantized = fake.astype(jnp.bfloat16)
    output = jnp.dot(normed, quantized, preferred_element_type=jnp.float32)
    misfit = (output - targets).astype(jnp.bfloat16)
    cotangent = lax.dot_general(normed, misfit, (((0,), (0,)), ((), ())), preferred_element_type=jnp.float32)
    return pullback(cotangent)

def reference(hidden, norm_gain, kv_weight, clip_upper, clip_lower):
    hidden_f = hidden.astype(jnp.float32)
    mean_sq = lax.optimization_barrier(jnp.mean(hidden_f * hidden_f, axis=1, keepdims=True))
    normed = (hidden_f * lax.rsqrt(mean_sq + norm_eps) * norm_gain.astype(jnp.float32)).astype(jnp.bfloat16)
    columns = kv_weight.shape[1]
    targets = jnp.dot(normed, kv_weight, preferred_element_type=jnp.float32)
    grouped = kv_weight.astype(jnp.float32).reshape(D // GROUP, GROUP, columns)
    magnitude = lax.optimization_barrier(jnp.max(jnp.abs(grouped), axis=1))
    param_count = 4 * (D // GROUP) * KVW
    upper, lower = (clip_upper, clip_lower)
    for iteration in range(STEPS):
        grad_up, grad_low = clip_gradients(upper, lower, grouped, magnitude, normed, targets)
        total_sq = jnp.sum(grad_up * grad_up) + jnp.sum(grad_low * grad_low)
        grad_rms = jnp.sqrt(total_sq / param_count + grad_eps)
        upper = upper - learn_rate * grad_up / grad_rms
        lower = lower - learn_rate * grad_low / grad_rms
    return (upper, lower)
```

```python
import functools
import math

import jax
import jax.numpy as jnp
from jax import lax
from jax.experimental import pallas as pl
from jax.experimental.pallas import tpu as pltpu
from jax.sharding import PartitionSpec as P

GROUP = 128
STEPS = 2
CHUNK = 8
LANES = 128

norm_eps = 1e-05
grad_eps = 1e-06
learn_rate = 0.25
top_level = 15.0

bf16, f32 = jnp.bfloat16, jnp.float32
ROUNDER = 12582912.0
SIN = (3.99733775, -10.17843475, 8.93899279)
COS = (0.99996212, -3.73207042, 4.98340402, -2.88721551)


def clip_params(upper, lower, magnitude):
    sig_up, sig_low = jax.nn.sigmoid(upper), jax.nn.sigmoid(lower)
    top, bottom = sig_up * magnitude, sig_low * magnitude
    step = (top + bottom + 1e-06) / top_level
    return sig_up, sig_low, top, bottom, step


def horner(x, coefs):
    acc = jnp.full_like(x, coefs[-1])
    for c in coefs[-2::-1]:
        acc = acc * x + jnp.asarray(c, x.dtype)
    return acc


def quantize_tile(w, low, high, inverse, zero, step):
    clipped = jnp.minimum(jnp.maximum(w.astype(f32), low), high)
    level = clipped * inverse + zero
    frac = (level - ((level + ROUNDER) - ROUNDER)).astype(bf16)
    x = frac * frac
    sine = frac * (jnp.asarray(0.25, bf16) - x) * horner(x, SIN)
    cosine = (jnp.asarray(1.0, bf16) - jnp.asarray(16.0, bf16) * x) * horner(x, COS)
    quantized = clipped.astype(bf16) - sine * step.astype(bf16)
    return quantized - w, quantized - (w - w * cosine), -cosine


def forward_kernel(w_ref, up_ref, low_ref, diff_ref, h1_ref, h2_ref, mag_ref, par_ref):
    chunk, columns = up_ref.shape
    for g in range(chunk):
        w = w_ref[g * GROUP : (g + 1) * GROUP, :]
        mag_ref[g : g + 1, :] = jnp.max(jnp.abs(w), axis=0, keepdims=True).astype(f32)
    _, _, top, bottom, step = clip_params(up_ref[...], low_ref[...], mag_ref[...])
    inverse = 1.0 / step
    par_ref[0] = -bottom
    par_ref[1] = top + 1e-06
    par_ref[2] = inverse
    par_ref[3] = bottom * inverse
    par_ref[4] = step

    for g in range(chunk):
        rows = pl.ds(g * GROUP, GROUP)
        for c in range(columns // LANES):
            lanes = pl.ds(c * LANES, LANES)
            par = [par_ref[k, g : g + 1, lanes] for k in range(5)]
            diff, h1, h2 = quantize_tile(w_ref[rows, lanes], *par)
            diff_ref[rows, lanes] = diff
            h1_ref[rows, lanes] = h1
            h2_ref[rows, lanes] = h2


def forward(weight, upper, lower):
    rows, columns = weight.shape
    groups = rows // GROUP
    big = pl.BlockSpec((CHUNK * GROUP, columns), lambda i: (i, 0))
    small = pl.BlockSpec((CHUNK, columns), lambda i: (i, 0))
    out = jax.ShapeDtypeStruct((rows, columns), bf16)
    return pl.pallas_call(
        forward_kernel,
        grid=(groups // CHUNK,),
        in_specs=[big, small, small],
        out_specs=[big, big, big, small],
        out_shape=[out, out, out, jax.ShapeDtypeStruct((groups, columns), f32)],
        scratch_shapes=[pltpu.VMEM((5, CHUNK, columns), f32)],
        cost_estimate=pl.CostEstimate(
            flops=30 * rows * columns, bytes_accessed=8 * rows * columns, transcendentals=0
        ),
    )(weight, upper, lower)


def backward_kernel(nt_ref, misfit_ref, h1_ref, h2_ref, up_ref, low_ref, mag_ref, grad_ref, sum_ref):
    chunk, columns = up_ref.shape
    for g in range(chunk):
        rows = pl.ds(g * GROUP, GROUP)
        cot = jnp.dot(nt_ref[rows, :], misfit_ref[...], preferred_element_type=f32)
        sum_ref[0, g : g + 1, :] = jnp.sum(cot * h1_ref[rows, :].astype(f32), axis=0, keepdims=True)
        sum_ref[1, g : g + 1, :] = jnp.sum(cot * h2_ref[rows, :].astype(f32), axis=0, keepdims=True)
    magnitude = mag_ref[...]
    sig_up, sig_low, top, bottom, step = clip_params(up_ref[...], low_ref[...], magnitude)
    t2 = sum_ref[1]
    grad_step = (sum_ref[0] - t2 * bottom) / step
    grad_top = grad_step / top_level
    grad_ref[0] = grad_top * magnitude * sig_up * (1.0 - sig_up)
    grad_ref[1] = (grad_top + t2) * magnitude * sig_low * (1.0 - sig_low)


def backward(normed_t, misfit, h1, h2, upper, lower, magnitude):
    rows, columns = h1.shape
    tokens = misfit.shape[0]
    groups = rows // GROUP
    big = pl.BlockSpec((CHUNK * GROUP, columns), lambda i: (i, 0))
    small = pl.BlockSpec((CHUNK, columns), lambda i: (i, 0))
    return pl.pallas_call(
        backward_kernel,
        grid=(groups // CHUNK,),
        in_specs=[
            pl.BlockSpec((CHUNK * GROUP, tokens), lambda i: (i, 0)),
            pl.BlockSpec((tokens, columns), lambda i: (0, 0)),
            big, big, small, small, small,
        ],
        out_specs=pl.BlockSpec((2, CHUNK, columns), lambda i: (0, i, 0)),
        out_shape=jax.ShapeDtypeStruct((2, groups, columns), f32),
        scratch_shapes=[pltpu.VMEM((2, CHUNK, columns), f32)],
        cost_estimate=pl.CostEstimate(
            flops=2 * tokens * rows * columns, bytes_accessed=5 * rows * columns, transcendentals=0
        ),
    )(normed_t, misfit, h1, h2, upper, lower, magnitude)


def body(hidden, norm_gain, kv_weight, clip_upper, clip_lower):
    gathered = lax.all_gather(hidden, "mp", axis=1, tiled=True)
    gathered_gain = lax.all_gather(norm_gain[None, :], "mp", axis=1, tiled=True)
    hidden_f = gathered.astype(f32)
    mean_sq = jnp.mean(hidden_f * hidden_f, axis=1, keepdims=True)
    normed = (hidden_f * lax.rsqrt(mean_sq + norm_eps) * gathered_gain[0].astype(f32)).astype(bf16)
    normed_t = normed.T
    groups = clip_upper.shape[0]
    param_count = 2 * groups * clip_upper.shape[1] * lax.axis_size("mp")
    share_rows = groups // lax.axis_size("dp")
    first_row = lax.axis_index("dp") * share_rows
    params = jnp.stack([clip_upper, clip_lower])
    for iteration in range(STEPS):
        diff, h1, h2, magnitude = forward(kv_weight, params[0], params[1])
        misfit = jnp.dot(normed, diff, preferred_element_type=f32).astype(bf16)
        grads = backward(normed_t, misfit, h1, h2, params[0], params[1], magnitude)
        if iteration + 1 < STEPS:
            grads = lax.psum(grads, "dp")
            total_sq = lax.psum(jnp.sum(grads * grads), "mp")
        else:
            grads = lax.psum_scatter(grads, "dp", scatter_dimension=1, tiled=True)
            total_sq = lax.psum(jnp.sum(grads * grads), ("dp", "mp"))
            params = lax.dynamic_slice_in_dim(params, first_row, share_rows, 1)
        grad_rms = jnp.sqrt(total_sq / param_count + grad_eps)
        params = params - learn_rate * grads / grad_rms
    return (params[0], params[1])


def solution(mesh):
    in_specs = (P("dp", "mp"), P("mp"), P(None, "mp"), P(None, "mp"), P(None, "mp"))
    out_specs = (P("dp", "mp"), P("dp", "mp"))
    return jax.shard_map(body, mesh=mesh, in_specs=in_specs, out_specs=out_specs, check_vma=False)
```

```python
import functools
import math

import jax
import jax.numpy as jnp
from jax import lax
from jax.experimental import pallas as pl
from jax.experimental.pallas import tpu as pltpu
from jax.sharding import PartitionSpec as P

GROUP = 128
STEPS = 2
CHUNK = 8
LANES = 128

norm_eps = 1e-05
grad_eps = 1e-06
learn_rate = 0.25
top_level = 15.0

bf16, f32 = jnp.bfloat16, jnp.float32
ROUNDER = 12582912.0
SIN = (3.99733775, -10.17843475, 8.93899279)
COS = (0.99996212, -3.73207042, 4.98340402, -2.88721551)


def clip_params(upper, lower, magnitude):
    sig_up, sig_low = jax.nn.sigmoid(upper), jax.nn.sigmoid(lower)
    top, bottom = sig_up * magnitude, sig_low * magnitude
    step = (top + bottom + 1e-06) / top_level
    return sig_up, sig_low, top, bottom, step


def horner(x, coefs):
    acc = jnp.full_like(x, coefs[-1])
    for c in coefs[-2::-1]:
        acc = acc * x + jnp.asarray(c, x.dtype)
    return acc


def quantize_tile(w, low, high, inverse, zero, step):
    clipped = jnp.minimum(jnp.maximum(w.astype(f32), low), high)
    level = clipped * inverse + zero
    frac = (level - ((level + ROUNDER) - ROUNDER)).astype(bf16)
    x = frac * frac
    sine = frac * (jnp.asarray(0.25, bf16) - x) * horner(x, SIN)
    cosine = (jnp.asarray(1.0, bf16) - jnp.asarray(16.0, bf16) * x) * horner(x, COS)
    quantized = clipped.astype(bf16) - sine * step.astype(bf16)
    return quantized - w, quantized - (w - w * cosine), -cosine


def forward_kernel(w_ref, up_ref, low_ref, diff_ref, h1_ref, h2_ref, mag_ref, par_ref):
    chunk, columns = up_ref.shape
    for g in range(chunk):
        w = w_ref[g * GROUP : (g + 1) * GROUP, :]
        mag_ref[g : g + 1, :] = jnp.max(jnp.abs(w), axis=0, keepdims=True).astype(f32)
    _, _, top, bottom, step = clip_params(up_ref[...], low_ref[...], mag_ref[...])
    inverse = 1.0 / step
    par_ref[0] = -bottom
    par_ref[1] = top + 1e-06
    par_ref[2] = inverse
    par_ref[3] = bottom * inverse
    par_ref[4] = step

    for g in range(chunk):
        rows = pl.ds(g * GROUP, GROUP)
        for c in range(columns // LANES):
            lanes = pl.ds(c * LANES, LANES)
            par = [par_ref[k, g : g + 1, lanes] for k in range(5)]
            diff, h1, h2 = quantize_tile(w_ref[rows, lanes], *par)
            diff_ref[rows, lanes] = diff
            h1_ref[rows, lanes] = h1
            h2_ref[rows, lanes] = h2


def forward(weight, upper, lower):
    rows, columns = weight.shape
    groups = rows // GROUP
    big = pl.BlockSpec((CHUNK * GROUP, columns), lambda i: (i, 0))
    small = pl.BlockSpec((CHUNK, columns), lambda i: (i, 0))
    out = jax.ShapeDtypeStruct((rows, columns), bf16)
    return pl.pallas_call(
        forward_kernel,
        grid=(groups // CHUNK,),
        in_specs=[big, small, small],
        out_specs=[big, big, big, small],
        out_shape=[out, out, out, jax.ShapeDtypeStruct((groups, columns), f32)],
        scratch_shapes=[pltpu.VMEM((5, CHUNK, columns), f32)],
        cost_estimate=pl.CostEstimate(
            flops=30 * rows * columns, bytes_accessed=8 * rows * columns, transcendentals=0
        ),
    )(weight, upper, lower)


def gather_kernel(hidden_ref, gain_ref, w_ref, up_ref, low_ref, diff_ref, h1_ref, h2_ref, mag_ref, all_ref, gains_ref, par_ref, gain_send, gain_recv, own_send, own_recv, far_send, far_recv, near_send, near_recv, local_sem):
    i, pieces = pl.program_id(0), pl.num_programs(0)
    m = lax.axis_size("mp")
    mine = lax.axis_index("mp")
    chip, core = mine // 2, lax.rem(mine, 2)
    chips = m // 2
    sibling = chip * 2 + 1 - core
    rows = hidden_ref.shape[0] // far_send.shape[1]

    def own_copies():
        copies = [
            pltpu.make_async_copy(hidden_ref, all_ref.at[mine], local_sem.at[0]),
            pltpu.make_async_copy(gain_ref, gains_ref.at[mine], local_sem.at[1]),
        ]
        for k in range(1, m):
            copies.append(
                pltpu.make_async_remote_copy(
                    src_ref=gain_ref, dst_ref=gains_ref.at[mine], send_sem=gain_send.at[k],
                    recv_sem=gain_recv.at[k], device_id={"mp": lax.rem(mine + k, m)},
                )
            )
        copies.append(
            pltpu.make_async_remote_copy(
                src_ref=hidden_ref, dst_ref=all_ref.at[mine], send_sem=own_send,
                recv_sem=own_recv, device_id={"mp": sibling},
            )
        )
        return copies

    def far_copy(k, p):
        span = pl.ds(p * rows, rows)
        return pltpu.make_async_remote_copy(
            src_ref=hidden_ref.at[span], dst_ref=all_ref.at[mine, span], send_sem=far_send.at[k, p],
            recv_sem=far_recv.at[k, p], device_id={"mp": lax.rem(chip + k, chips) * 2 + core},
        )

    def near_copy(k, p):
        span = pl.ds(p * rows, rows)
        source = lax.rem(chip + chips - k, chips) * 2 + core
        return pltpu.make_async_remote_copy(
            src_ref=all_ref.at[source, span], dst_ref=all_ref.at[source, span],
            send_sem=near_send.at[k, p], recv_sem=near_recv.at[k, p], device_id={"mp": sibling},
        )

    @pl.when(i == 0)
    def _():
        barrier = pltpu.get_barrier_semaphore()
        for k in range(1, m):
            pl.semaphore_signal(barrier, inc=1, device_id={"mp": lax.rem(mine + k, m)})
        pl.semaphore_wait(barrier, m - 1)
        for p in range(far_send.shape[1]):
            for k in range(1, chips):
                far_copy(k, p).start()
        for copy in own_copies():
            copy.start()

    forward_kernel(w_ref, up_ref, low_ref, diff_ref, h1_ref, h2_ref, mag_ref, par_ref)

    for k in range(1, chips):
        far_copy(k, i).wait_recv()
        near_copy(k, i).start()

    @pl.when(i == pieces - 1)
    def _():
        for copy in own_copies():
            copy.wait()
        for p in range(far_send.shape[1]):
            for k in range(1, chips):
                far_copy(k, p).wait_send()
                near_copy(k, p).wait()


def gather_forward(hidden, gain, weight, upper, lower):
    rows, columns = weight.shape
    groups = rows // GROUP
    m = lax.axis_size("mp")
    pieces = groups // CHUNK
    gain = gain.reshape(-1, LANES)
    big = pl.BlockSpec((CHUNK * GROUP, columns), lambda i: (i, 0))
    small = pl.BlockSpec((CHUNK, columns), lambda i: (i, 0))
    out = jax.ShapeDtypeStruct((rows, columns), bf16)
    dma = pltpu.SemaphoreType.DMA
    return pl.pallas_call(
        gather_kernel,
        grid=(pieces,),
        in_specs=[
            pl.BlockSpec(hidden.shape, lambda i: (0, 0)),
            pl.BlockSpec(gain.shape, lambda i: (0, 0)),
            big, small, small,
        ],
        out_specs=[big, big, big, small, pl.BlockSpec(memory_space=pl.ANY), pl.BlockSpec(memory_space=pl.ANY)],
        out_shape=[
            out, out, out, jax.ShapeDtypeStruct((groups, columns), f32),
            jax.ShapeDtypeStruct((m,) + hidden.shape, bf16),
            jax.ShapeDtypeStruct((m,) + gain.shape, bf16),
        ],
        scratch_shapes=[
            pltpu.VMEM((5, CHUNK, columns), f32),
            dma((m,)), dma((m,)), dma, dma,
            dma((m // 2, pieces)), dma((m // 2, pieces)), dma((m // 2, pieces)), dma((m // 2, pieces)),
            dma((2,)),
        ],
        compiler_params=pltpu.CompilerParams(collective_id=2, has_side_effects=True),
    )(hidden, gain, weight, upper, lower)


def backward_kernel(nt_ref, misfit_ref, h1_ref, h2_ref, up_ref, low_ref, mag_ref, grad_ref, sum_ref):
    chunk, columns = up_ref.shape
    for g in range(chunk):
        rows = pl.ds(g * GROUP, GROUP)
        cot = jnp.dot(nt_ref[rows, :], misfit_ref[...], preferred_element_type=f32)
        sum_ref[0, g : g + 1, :] = jnp.sum(cot * h1_ref[rows, :].astype(f32), axis=0, keepdims=True)
        sum_ref[1, g : g + 1, :] = jnp.sum(cot * h2_ref[rows, :].astype(f32), axis=0, keepdims=True)
    magnitude = mag_ref[...]
    sig_up, sig_low, top, bottom, step = clip_params(up_ref[...], low_ref[...], magnitude)
    t2 = sum_ref[1]
    grad_step = (sum_ref[0] - t2 * bottom) / step
    grad_top = grad_step / top_level
    grad_ref[0] = grad_top * magnitude * sig_up * (1.0 - sig_up)
    grad_ref[1] = (grad_top + t2) * magnitude * sig_low * (1.0 - sig_low)


def backward(normed_t, misfit, h1, h2, upper, lower, magnitude):
    rows, columns = h1.shape
    tokens = misfit.shape[0]
    groups = rows // GROUP
    big = pl.BlockSpec((CHUNK * GROUP, columns), lambda i: (i, 0))
    small = pl.BlockSpec((CHUNK, columns), lambda i: (i, 0))
    return pl.pallas_call(
        backward_kernel,
        grid=(groups // CHUNK,),
        in_specs=[
            pl.BlockSpec((CHUNK * GROUP, tokens), lambda i: (i, 0)),
            pl.BlockSpec((tokens, columns), lambda i: (0, 0)),
            big, big, small, small, small,
        ],
        out_specs=pl.BlockSpec((2, CHUNK, columns), lambda i: (0, i, 0)),
        out_shape=jax.ShapeDtypeStruct((2, groups, columns), f32),
        scratch_shapes=[pltpu.VMEM((2, CHUNK, columns), f32)],
        cost_estimate=pl.CostEstimate(
            flops=2 * tokens * rows * columns, bytes_accessed=5 * rows * columns, transcendentals=0
        ),
    )(normed_t, misfit, h1, h2, upper, lower, magnitude)


def update_kernel(last, count, grads_ref, params_ref, out_ref, parts, sums, squares, totals, send1, recv1, send2, recv2, send3, recv3):
    n, m = lax.axis_size("dp"), lax.axis_size("mp")
    me, mine = lax.axis_index("dp"), lax.axis_index("mp")

    def peer(axis, size, index, k):
        return {axis: lax.rem(index + k, size)}

    barrier = pltpu.get_barrier_semaphore()
    for k in range(1, n):
        pl.semaphore_signal(barrier, inc=1, device_id=peer("dp", n, me, k))
    for k in range(1, m):
        pl.semaphore_signal(barrier, inc=1, device_id=peer("mp", m, mine, k))
    pl.semaphore_wait(barrier, n + m - 2)

    def exchange(axis, size, index, source, dest, send, recv):
        copies = []
        for k in range(1, size):
            copies.append(
                pltpu.make_async_remote_copy(
                    src_ref=source(k), dst_ref=dest(k), send_sem=send.at[k], recv_sem=recv.at[k],
                    device_id=peer(axis, size, index, k),
                )
            )
            copies[-1].start()
        return copies

    copies = exchange(
        "dp", n, me, lambda k: grads_ref.at[lax.rem(me + k, n)], lambda k: parts.at[k], send1, recv1
    )
    total = grads_ref[me]
    for k, copy in enumerate(copies, 1):
        copy.wait_recv()
        total = total + parts[k]
    columns = total.shape[1]
    lanes = jnp.sum((total * total).reshape(-1, columns // LANES, LANES), axis=(0, 1))[None]
    mine_sq = jnp.broadcast_to(lanes, (8, LANES))
    if last:
        squares[0] = mine_sq
        gathers = exchange("dp", n, me, lambda k: squares.at[0], lambda k: squares.at[k], send2, recv2)
    else:
        sums[0] = total
        gathers = exchange("dp", n, me, lambda k: sums.at[0], lambda k: sums.at[k], send2, recv2)
    square = mine_sq
    for k, copy in enumerate(gathers, 1):
        copy.wait_recv()
        if last:
            square = square + squares[k]
        else:
            part = sums[k] * sums[k]
            square = square + jnp.broadcast_to(
                jnp.sum(part.reshape(-1, columns // LANES, LANES), axis=(0, 1))[None], (8, LANES)
            )
    totals[0] = square
    finals = exchange("mp", m, mine, lambda k: totals.at[0], lambda k: totals.at[k], send3, recv3)
    for k, copy in enumerate(finals, 1):
        copy.wait_recv()
        square = square + totals[k]
    total_sq = jnp.sum(square[0:1], axis=1, keepdims=True)
    scale = learn_rate / jnp.sqrt(total_sq / count + grad_eps)
    if last:
        out_ref[...] = params_ref[me] - scale * total
    else:
        out_ref[me] = params_ref[me] - scale * total
        for k in range(1, n):
            owner = lax.rem(me + n - k, n)
            out_ref[owner] = params_ref[owner] - scale * sums[k]
    for copy in copies + gathers + finals:
        copy.wait_send()


def update(last, count, grads, params):
    n, rows, columns = grads.shape
    m = lax.axis_size("mp")
    whole = pl.BlockSpec(memory_space=pltpu.VMEM)
    dma = pltpu.SemaphoreType.DMA
    return pl.pallas_call(
        functools.partial(update_kernel, last, count),
        in_specs=[whole, whole],
        out_specs=whole,
        out_shape=jax.ShapeDtypeStruct((rows, columns) if last else (n, rows, columns), f32),
        scratch_shapes=[
            pltpu.VMEM((n, rows, columns), f32),
            pltpu.VMEM((n, rows, columns), f32),
            pltpu.VMEM((n, 8, LANES), f32),
            pltpu.VMEM((m, 8, LANES), f32),
            dma((n,)), dma((n,)), dma((n,)), dma((n,)), dma((m,)), dma((m,)),
        ],
        compiler_params=pltpu.CompilerParams(collective_id=1 if last else 0, has_side_effects=True),
    )(grads, params)


def pack(arrays, share):
    _, groups, columns = arrays.shape
    split = arrays.reshape(2, groups // share, share, columns)
    return split.transpose(1, 0, 2, 3).reshape(groups // share, 2 * share, columns)


def unpack(packed, share):
    parts, _, columns = packed.shape
    split = packed.reshape(parts, 2, share, columns).transpose(1, 0, 2, 3)
    return split.reshape(2, parts * share, columns)


def body(hidden, norm_gain, kv_weight, clip_upper, clip_lower):
    *first, blocks, gains = gather_forward(hidden, norm_gain, kv_weight, clip_upper, clip_lower)
    hidden_f = blocks.astype(f32)
    m, tokens, features = blocks.shape
    mean_sq = jnp.sum(hidden_f * hidden_f, axis=(0, 2), keepdims=True) / (m * features)
    scaled = hidden_f * lax.rsqrt(mean_sq + norm_eps) * gains.reshape(m, 1, features).astype(f32)
    normed_t = scaled.astype(bf16).transpose(0, 2, 1).reshape(m * features, tokens)
    groups = clip_upper.shape[0]
    param_count = 2 * groups * clip_upper.shape[1] * lax.axis_size("mp")
    share = groups // lax.axis_size("dp")
    packed = pack(jnp.stack([clip_upper, clip_lower]), share)
    upper, lower = clip_upper, clip_lower
    for iteration in range(STEPS):
        if iteration == 0:
            diff, h1, h2, magnitude = first
        else:
            diff, h1, h2, magnitude = forward(kv_weight, upper, lower)
        misfit = lax.dot_general(
            normed_t, diff, (((0,), (0,)), ((), ())), preferred_element_type=f32
        ).astype(bf16)
        grads = pack(backward(normed_t, misfit, h1, h2, upper, lower, magnitude), share)
        last = iteration + 1 == STEPS
        packed = update(last, param_count, grads, packed)
        if not last:
            upper, lower = unpack(packed, share)
    return (packed[:share], packed[share:])


def solution(mesh):
    in_specs = (P("dp", "mp"), P("mp"), P(None, "mp"), P(None, "mp"), P(None, "mp"))
    out_specs = (P("dp", "mp"), P("dp", "mp"))
    return jax.shard_map(body, mesh=mesh, in_specs=in_specs, out_specs=out_specs, check_vma=False)
```

```python
import functools
import math

import jax
import jax.numpy as jnp
from jax import lax
from jax.experimental import pallas as pl
from jax.experimental.pallas import tpu as pltpu
from jax.sharding import PartitionSpec as P

GROUP = 128
STEPS = 2
CHUNK = 8
LANES = 128

norm_eps = 1e-05
grad_eps = 1e-06
learn_rate = 0.25
top_level = 15.0

bf16, f32 = jnp.bfloat16, jnp.float32
ROUNDER = 12582912.0
SIN = (3.99733775, -10.17843475, 8.93899279)
COS = (0.99996212, -3.73207042, 4.98340402, -2.88721551)


def clip_params(upper, lower, magnitude):
    sig_up, sig_low = jax.nn.sigmoid(upper), jax.nn.sigmoid(lower)
    top, bottom = sig_up * magnitude, sig_low * magnitude
    step = (top + bottom + 1e-06) / top_level
    return sig_up, sig_low, top, bottom, step


def horner(x, coefs):
    acc = jnp.full_like(x, coefs[-1])
    for c in coefs[-2::-1]:
        acc = acc * x + jnp.asarray(c, x.dtype)
    return acc


def quantize_tile(w, low, high, inverse, zero, step):
    clipped = jnp.minimum(jnp.maximum(w.astype(f32), low), high)
    level = clipped * inverse + zero
    frac = (level - ((level + ROUNDER) - ROUNDER)).astype(bf16)
    x = frac * frac
    sine = frac * (jnp.asarray(0.25, bf16) - x) * horner(x, SIN)
    cosine = (jnp.asarray(1.0, bf16) - jnp.asarray(16.0, bf16) * x) * horner(x, COS)
    quantized = clipped.astype(bf16) - sine * step.astype(bf16)
    return quantized - w, quantized - (w - w * cosine), -cosine


def forward_kernel(w_ref, up_ref, low_ref, diff_ref, h1_ref, h2_ref, mag_ref, par_ref):
    chunk, columns = up_ref.shape
    for g in range(chunk):
        w = w_ref[g * GROUP : (g + 1) * GROUP, :]
        mag_ref[g : g + 1, :] = jnp.max(jnp.abs(w), axis=0, keepdims=True).astype(f32)
    _, _, top, bottom, step = clip_params(up_ref[...], low_ref[...], mag_ref[...])
    inverse = 1.0 / step
    par_ref[0] = -bottom
    par_ref[1] = top + 1e-06
    par_ref[2] = inverse
    par_ref[3] = bottom * inverse
    par_ref[4] = step

    for g in range(chunk):
        rows = pl.ds(g * GROUP, GROUP)
        for c in range(columns // LANES):
            lanes = pl.ds(c * LANES, LANES)
            par = [par_ref[k, g : g + 1, lanes] for k in range(5)]
            diff, h1, h2 = quantize_tile(w_ref[rows, lanes], *par)
            diff_ref[rows, lanes] = diff
            h1_ref[rows, lanes] = h1
            h2_ref[rows, lanes] = h2


def forward(weight, upper, lower):
    rows, columns = weight.shape
    groups = rows // GROUP
    big = pl.BlockSpec((CHUNK * GROUP, columns), lambda i: (i, 0))
    small = pl.BlockSpec((CHUNK, columns), lambda i: (i, 0))
    out = jax.ShapeDtypeStruct((rows, columns), bf16)
    return pl.pallas_call(
        forward_kernel,
        grid=(groups // CHUNK,),
        in_specs=[big, small, small],
        out_specs=[big, big, big, small],
        out_shape=[out, out, out, jax.ShapeDtypeStruct((groups, columns), f32)],
        scratch_shapes=[pltpu.VMEM((5, CHUNK, columns), f32)],
        cost_estimate=pl.CostEstimate(
            flops=30 * rows * columns, bytes_accessed=8 * rows * columns, transcendentals=0
        ),
    )(weight, upper, lower)


def gather_kernel(hidden_ref, gain_ref, w_ref, up_ref, low_ref, diff_ref, h1_ref, h2_ref, mag_ref, all_ref, gains_ref, par_ref, gain_send, gain_recv, own_send, own_recv, far_send, far_recv, near_send, near_recv, local_sem):
    i, pieces = pl.program_id(0), pl.num_programs(0)
    m = lax.axis_size("mp")
    mine = lax.axis_index("mp")
    chip, core = mine // 2, lax.rem(mine, 2)
    chips = m // 2
    sibling = chip * 2 + 1 - core
    rows = hidden_ref.shape[0] // far_send.shape[1]

    features = hidden_ref.shape[1]

    def place(source):
        return pl.ds(pl.multiple_of(source * features, LANES), features)

    def own_copies():
        copies = [
            pltpu.make_async_copy(hidden_ref, all_ref.at[:, place(mine)], local_sem.at[0]),
            pltpu.make_async_copy(gain_ref, gains_ref.at[mine], local_sem.at[1]),
        ]
        for k in range(1, m):
            copies.append(
                pltpu.make_async_remote_copy(
                    src_ref=gain_ref, dst_ref=gains_ref.at[mine], send_sem=gain_send.at[k],
                    recv_sem=gain_recv.at[k], device_id={"mp": lax.rem(mine + k, m)},
                )
            )
        copies.append(
            pltpu.make_async_remote_copy(
                src_ref=hidden_ref, dst_ref=all_ref.at[:, place(mine)], send_sem=own_send,
                recv_sem=own_recv, device_id={"mp": sibling},
            )
        )
        return copies

    def far_copy(k, p):
        span = pl.ds(p * rows, rows)
        return pltpu.make_async_remote_copy(
            src_ref=hidden_ref.at[span], dst_ref=all_ref.at[span, place(mine)], send_sem=far_send.at[k, p],
            recv_sem=far_recv.at[k, p], device_id={"mp": lax.rem(chip + k, chips) * 2 + core},
        )

    def near_copy(k, p):
        span = pl.ds(p * rows, rows)
        source = lax.rem(chip + chips - k, chips) * 2 + core
        return pltpu.make_async_remote_copy(
            src_ref=all_ref.at[span, place(source)], dst_ref=all_ref.at[span, place(source)],
            send_sem=near_send.at[k, p], recv_sem=near_recv.at[k, p], device_id={"mp": sibling},
        )

    @pl.when(i == 0)
    def _():
        barrier = pltpu.get_barrier_semaphore()
        for k in range(1, m):
            pl.semaphore_signal(barrier, inc=1, device_id={"mp": lax.rem(mine + k, m)})
        pl.semaphore_wait(barrier, m - 1)
        for p in range(far_send.shape[1]):
            for k in range(1, chips):
                far_copy(k, p).start()
        for copy in own_copies():
            copy.start()

    forward_kernel(w_ref, up_ref, low_ref, diff_ref, h1_ref, h2_ref, mag_ref, par_ref)

    for k in range(1, chips):
        far_copy(k, i).wait_recv()
        near_copy(k, i).start()

    @pl.when(i == pieces - 1)
    def _():
        for copy in own_copies():
            copy.wait()
        for p in range(far_send.shape[1]):
            for k in range(1, chips):
                far_copy(k, p).wait_send()
                near_copy(k, p).wait()


def gather_forward(hidden, gain, weight, upper, lower):
    rows, columns = weight.shape
    groups = rows // GROUP
    m = lax.axis_size("mp")
    pieces = groups // CHUNK
    gain = gain.reshape(-1, LANES)
    big = pl.BlockSpec((CHUNK * GROUP, columns), lambda i: (i, 0))
    small = pl.BlockSpec((CHUNK, columns), lambda i: (i, 0))
    out = jax.ShapeDtypeStruct((rows, columns), bf16)
    dma = pltpu.SemaphoreType.DMA
    return pl.pallas_call(
        gather_kernel,
        grid=(pieces,),
        in_specs=[
            pl.BlockSpec(hidden.shape, lambda i: (0, 0)),
            pl.BlockSpec(gain.shape, lambda i: (0, 0)),
            big, small, small,
        ],
        out_specs=[big, big, big, small, pl.BlockSpec(memory_space=pl.ANY), pl.BlockSpec(memory_space=pl.ANY)],
        out_shape=[
            out, out, out, jax.ShapeDtypeStruct((groups, columns), f32),
            jax.ShapeDtypeStruct((hidden.shape[0], m * hidden.shape[1]), bf16),
            jax.ShapeDtypeStruct((m,) + gain.shape, bf16),
        ],
        scratch_shapes=[
            pltpu.VMEM((5, CHUNK, columns), f32),
            dma((m,)), dma((m,)), dma, dma,
            dma((m // 2, pieces)), dma((m // 2, pieces)), dma((m // 2, pieces)), dma((m // 2, pieces)),
            dma((2,)),
        ],
        compiler_params=pltpu.CompilerParams(collective_id=2, has_side_effects=True),
    )(hidden, gain, weight, upper, lower)


def backward_kernel(nt_ref, misfit_ref, h1_ref, h2_ref, up_ref, low_ref, mag_ref, grad_ref, sum_ref):
    chunk, columns = up_ref.shape
    for g in range(chunk):
        rows = pl.ds(g * GROUP, GROUP)
        cot = jnp.dot(nt_ref[rows, :], misfit_ref[...], preferred_element_type=f32)
        sum_ref[0, g : g + 1, :] = jnp.sum(cot * h1_ref[rows, :].astype(f32), axis=0, keepdims=True)
        sum_ref[1, g : g + 1, :] = jnp.sum(cot * h2_ref[rows, :].astype(f32), axis=0, keepdims=True)
    magnitude = mag_ref[...]
    sig_up, sig_low, top, bottom, step = clip_params(up_ref[...], low_ref[...], magnitude)
    t2 = sum_ref[1]
    grad_step = (sum_ref[0] - t2 * bottom) / step
    grad_top = grad_step / top_level
    grad_ref[0] = grad_top * magnitude * sig_up * (1.0 - sig_up)
    grad_ref[1] = (grad_top + t2) * magnitude * sig_low * (1.0 - sig_low)


def backward(normed_t, misfit, h1, h2, upper, lower, magnitude):
    rows, columns = h1.shape
    tokens = misfit.shape[0]
    groups = rows // GROUP
    big = pl.BlockSpec((CHUNK * GROUP, columns), lambda i: (i, 0))
    small = pl.BlockSpec((CHUNK, columns), lambda i: (i, 0))
    return pl.pallas_call(
        backward_kernel,
        grid=(groups // CHUNK,),
        in_specs=[
            pl.BlockSpec((CHUNK * GROUP, tokens), lambda i: (i, 0)),
            pl.BlockSpec((tokens, columns), lambda i: (0, 0)),
            big, big, small, small, small,
        ],
        out_specs=pl.BlockSpec((2, CHUNK, columns), lambda i: (0, i, 0)),
        out_shape=jax.ShapeDtypeStruct((2, groups, columns), f32),
        scratch_shapes=[pltpu.VMEM((2, CHUNK, columns), f32)],
        cost_estimate=pl.CostEstimate(
            flops=2 * tokens * rows * columns, bytes_accessed=5 * rows * columns, transcendentals=0
        ),
    )(normed_t, misfit, h1, h2, upper, lower, magnitude)


def update_kernel(last, count, grads_ref, params_ref, out_ref, parts, sums, squares, totals, send1, recv1, send2, recv2, send3, recv3):
    n, m = lax.axis_size("dp"), lax.axis_size("mp")
    me, mine = lax.axis_index("dp"), lax.axis_index("mp")

    def peer(axis, size, index, k):
        return {axis: lax.rem(index + k, size)}

    barrier = pltpu.get_barrier_semaphore()
    for k in range(1, n):
        pl.semaphore_signal(barrier, inc=1, device_id=peer("dp", n, me, k))
    for k in range(1, m):
        pl.semaphore_signal(barrier, inc=1, device_id=peer("mp", m, mine, k))
    pl.semaphore_wait(barrier, n + m - 2)

    def exchange(axis, size, index, source, dest, send, recv):
        copies = []
        for k in range(1, size):
            copies.append(
                pltpu.make_async_remote_copy(
                    src_ref=source(k), dst_ref=dest(k), send_sem=send.at[k], recv_sem=recv.at[k],
                    device_id=peer(axis, size, index, k),
                )
            )
            copies[-1].start()
        return copies

    copies = exchange(
        "dp", n, me, lambda k: grads_ref.at[lax.rem(me + k, n)], lambda k: parts.at[k], send1, recv1
    )
    total = grads_ref[me].astype(f32)
    for k, copy in enumerate(copies, 1):
        copy.wait_recv()
        total = total + parts[k].astype(f32)
    columns = total.shape[1]
    lanes = jnp.sum((total * total).reshape(-1, columns // LANES, LANES), axis=(0, 1))[None]
    mine_sq = jnp.broadcast_to(lanes, (8, LANES))
    if last:
        squares[0] = mine_sq
        gathers = exchange("dp", n, me, lambda k: squares.at[0], lambda k: squares.at[k], send2, recv2)
    else:
        sums[0] = total
        gathers = exchange("dp", n, me, lambda k: sums.at[0], lambda k: sums.at[k], send2, recv2)
    square = mine_sq
    for k, copy in enumerate(gathers, 1):
        copy.wait_recv()
        if last:
            square = square + squares[k]
        else:
            part = sums[k] * sums[k]
            square = square + jnp.broadcast_to(
                jnp.sum(part.reshape(-1, columns // LANES, LANES), axis=(0, 1))[None], (8, LANES)
            )
    totals[0] = square
    finals = exchange("mp", m, mine, lambda k: totals.at[0], lambda k: totals.at[k], send3, recv3)
    for k, copy in enumerate(finals, 1):
        copy.wait_recv()
        square = square + totals[k]
    total_sq = jnp.sum(square[0:1], axis=1, keepdims=True)
    scale = learn_rate / jnp.sqrt(total_sq / count + grad_eps)
    if last:
        out_ref[...] = params_ref[me] - scale * total
    else:
        out_ref[me] = params_ref[me] - scale * total
        for k in range(1, n):
            owner = lax.rem(me + n - k, n)
            out_ref[owner] = params_ref[owner] - scale * sums[k]
    for copy in copies + gathers + finals:
        copy.wait_send()


def update(last, count, grads, params):
    n, rows, columns = grads.shape
    m = lax.axis_size("mp")
    whole = pl.BlockSpec(memory_space=pltpu.VMEM)
    dma = pltpu.SemaphoreType.DMA
    return pl.pallas_call(
        functools.partial(update_kernel, last, count),
        in_specs=[whole, whole],
        out_specs=whole,
        out_shape=jax.ShapeDtypeStruct((rows, columns) if last else (n, rows, columns), f32),
        scratch_shapes=[
            pltpu.VMEM((n, rows, columns), bf16),
            pltpu.VMEM((n, rows, columns), f32),
            pltpu.VMEM((n, 8, LANES), f32),
            pltpu.VMEM((m, 8, LANES), f32),
            dma((n,)), dma((n,)), dma((n,)), dma((n,)), dma((m,)), dma((m,)),
        ],
        compiler_params=pltpu.CompilerParams(collective_id=1 if last else 0, has_side_effects=True),
    )(grads, params)


def pack(arrays, share):
    _, groups, columns = arrays.shape
    split = arrays.reshape(2, groups // share, share, columns)
    return split.transpose(1, 0, 2, 3).reshape(groups // share, 2 * share, columns)


def unpack(packed, share):
    parts, _, columns = packed.shape
    split = packed.reshape(parts, 2, share, columns).transpose(1, 0, 2, 3)
    return split.reshape(2, parts * share, columns)


def body(hidden, norm_gain, kv_weight, clip_upper, clip_lower):
    *first, blocks, gains = gather_forward(hidden, norm_gain, kv_weight, clip_upper, clip_lower)
    hidden_f = blocks.astype(f32)
    mean_sq = jnp.mean(hidden_f * hidden_f, axis=1, keepdims=True)
    normed = (hidden_f * lax.rsqrt(mean_sq + norm_eps) * gains.reshape(1, -1).astype(f32)).astype(bf16)
    normed_t = normed.T
    groups = clip_upper.shape[0]
    param_count = 2 * groups * clip_upper.shape[1] * lax.axis_size("mp")
    share = groups // lax.axis_size("dp")
    packed = pack(jnp.stack([clip_upper, clip_lower]), share)
    upper, lower = clip_upper, clip_lower
    for iteration in range(STEPS):
        if iteration == 0:
            diff, h1, h2, magnitude = first
        else:
            diff, h1, h2, magnitude = forward(kv_weight, upper, lower)
        misfit = jnp.dot(normed, diff, preferred_element_type=f32).astype(bf16)
        grads = pack(backward(normed_t, misfit, h1, h2, upper, lower, magnitude), share).astype(bf16)
        last = iteration + 1 == STEPS
        packed = update(last, param_count, grads, packed)
        if not last:
            upper, lower = unpack(packed, share)
    return (packed[:share], packed[share:])


def solution(mesh):
    in_specs = (P("dp", "mp"), P("mp"), P(None, "mp"), P(None, "mp"), P(None, "mp"))
    out_specs = (P("dp", "mp"), P("dp", "mp"))
    return jax.shard_map(body, mesh=mesh, in_specs=in_specs, out_specs=out_specs, check_vma=False)
```
